32 devices in a mesh: dp: 8 (over z, core), mp: 4 (over y, x).
Axes of the slice: x: 2, y: 2, z: 4, core: 2. Of those that a mesh axis runs over, the one named last changes fastest.
Arguments:
- master: float32 [4096, 5120], P('dp', 'mp'), may hold values from -60 to 60
- moment_first: float32 [4096, 5120], P('dp', 'mp'), may hold values from -0.06 to 0.06
- moment_second: float32 [4096, 5120], P('dp', 'mp'), may hold values from 1e-05 to 0.001
- gradients: float32 [4096, 5120], P('dp', 'mp'), may hold values from -0.2 to 0.2
- step_count: int32 [1], replicated, may hold values from 1 to 10
- tensor_rows: int32 [24], replicated, may hold values from 1 to 1024, 4096 in all
- decay_mask: int32 [24], replicated, may hold values 0 or 1
Outputs:
- new_master: float32 [4096, 5120], P('dp', 'mp')
- new_first: float32 [4096, 5120], P('dp', 'mp')
- new_second: float32 [4096, 5120], P('dp', 'mp')
- compute_weights: bfloat16 [4096, 5120], P(None, 'mp')
The draws below stay inside these ranges and needn't reach their ends.
Inputs may be any that keep to these rules, and one draw needn't show every extreme that they name: `tensor_rows`: the rows sum to 4096; the largest tensor has 1024 rows.
All inputs are finite; a program needn't handle non-finite values.
Results may differ from the reference program's by a relative error of at most 0.0004.
Values may be sent and summed in bfloat16 or wider, within the bound.
No kernel may reach another device: no remote copies, remote signals or barrier semaphores. Data moves between devices by JAX's collectives and lax.ppermute only.
A program may use at most 128 MiB of HBM per device.

```python
import math
import jax
import jax.numpy as jnp
import numpy as np
from jax import lax

WIDE = 5120
TENSORS = 24
ROWS = 4096
MOST = 1024


def draw_master(key, part):
    keys = jax.random.split(key, 3)
    row_scale = jnp.exp(jax.random.uniform(keys[0], (ROWS, 1), jnp.float32, -1.2, 1.2))
    col_scale = jnp.exp(jax.random.uniform(keys[1], (1, WIDE), jnp.float32, -1.2, 1.2))
    ramp = 1.0 + 2.0 * jnp.arange(ROWS, dtype=jnp.float32)[:, None] / ROWS
    base = jax.random.normal(keys[2], (ROWS, WIDE), jnp.float32)
    values = 0.3 * base * row_scale * col_scale * ramp
    return jnp.clip(values, -60.0, 60.0).astype(jnp.float32)


def set_ends(entries, key, low, top_value):
    longest = entries.shape.index(max(entries.shape))
    spots = []
    for shift in (0, 1):
        where = [jax.random.randint(jax.random.fold_in(key, axis), (), 0, length) for axis, length in enumerate(entries.shape)]
        where[longest] = (where[longest] + shift) % entries.shape[longest]
        spots.append(tuple(where))
    return entries.at[spots[0]].set(low).at[spots[1]].set(top_value)


def block_levels(own_key, dims, shards, low, high):
    level = 1.0
    for axis_at, shards_of in shards:
        draws = jax.random.uniform(jax.random.fold_in(jax.random.fold_in(own_key, 6), axis_at), (shards_of,), jnp.float32, low / len(shards), high / len(shards))
        level = level * jnp.repeat(jnp.exp(draws), dims[axis_at] // shards_of).reshape((-1,) + (1,) * (len(dims) - 1 - axis_at))
    return level


def profile(count, total, limit, slope):
    loads = [(1 << 20) // math.isqrt(grade ** slope) + 1 for grade in range(2, count + 1)]
    rest, counts = total - limit - (count - 1), [1] * (count - 1)
    while rest > 0:
        movable = [i for i in range(count - 1) if counts[i] < limit]
        pool, budget = sum([loads[i] for i in movable]), rest
        for i in movable:
            more = min(limit - counts[i], max(1, budget * loads[i] // pool), rest)
            counts[i] = counts[i] + more
            rest = rest - more
    return np.array([limit] + counts)


def ragged_sizes(stream_key, amount, total, most, slope):
    if amount == 2:
        one = jax.random.randint(stream_key, (), max(1, total - most), min(most, total - 1) + 1)
        return jnp.stack([one, total - one])
    tallies = jnp.asarray(profile(amount, total, most, slope), jnp.int32)
    pairs = (amount - 1) // 2
    source_of, taker = tallies[1:1 + 2 * pairs:2], tallies[2:2 + 2 * pairs:2]
    room = jnp.minimum(source_of - 1, most - taker)
    shifted = jax.random.randint(jax.random.fold_in(stream_key, 1), (pairs,), 0, 1 << 20) % (room + 1)
    tallies = tallies.at[1:1 + 2 * pairs:2].set(source_of - shifted).at[2:2 + 2 * pairs:2].set(taker + shifted)
    return tallies[jax.random.permutation(jax.random.fold_in(stream_key, 2), amount)]


def bell_draw(key, dims, width, bound, cuts=(), held_as=jnp.bfloat16):
    gain = block_levels(key, dims, cuts, -0.22, 0.18) if cuts else 1.0
    values = jax.random.normal(key, dims, jnp.float32) * width * gain
    return jnp.minimum(jnp.maximum(values, -bound), bound).astype(held_as)


def setup_inputs(seed: int = 0) -> dict:
    arg_keys = jax.random.split(jax.random.key(seed), 8)
    master = draw_master(jax.random.fold_in(arg_keys[7], 71), 0)
    moment_first = bell_draw(arg_keys[1], (ROWS, WIDE), 0.01, 0.06, ((0, 8), (1, 4)), jnp.float32)
    moment_second = jnp.clip(jnp.exp(math.log(0.001) - 4.6051703 * jax.random.uniform(arg_keys[2], (ROWS, WIDE), jnp.float32) ** block_levels(arg_keys[2], (ROWS, WIDE), ((0, 8), (1, 4)), -0.2, 0.2)), 9.999999747378752e-06, 0.001)
    gradients = bell_draw(arg_keys[3], (ROWS, WIDE), 0.03, 0.2, ((0, 8), (1, 4)), jnp.float32)
    step_count = jax.random.randint(arg_keys[4], (1,), 1, 11).astype(jnp.int32)
    tensor_rows = ragged_sizes(arg_keys[5], TENSORS, ROWS, MOST, 1).astype(jnp.int32)
    decay_mask = set_ends((jax.random.randint(arg_keys[6], (TENSORS,), 0, 2) < 1).astype(jnp.int32), jax.random.fold_in(arg_keys[6], 1), 0, 1)
    return dict(master=master, moment_first=moment_first, moment_second=moment_second, gradients=gradients, step_count=step_count, tensor_rows=tensor_rows, decay_mask=decay_mask)


beta_first = 0.9
beta_second = 0.999
adam_epsilon = 1e-06
decay_rate = 0.3
learn_rate = 0.3
norm_epsilon = 1e-06

def reference(master, moment_first, moment_second, gradients, step_count, tensor_rows, decay_mask):
    steps = step_count[0].astype(jnp.float32)
    new_first = beta_first * moment_first + (1.0 - beta_first) * gradients
    new_second = beta_second * moment_second + (1.0 - beta_second) * gradients * gradients
    fix_first = 1.0 - jnp.power(jnp.float32(beta_first), steps)
    fix_second = 1.0 - jnp.power(jnp.float32(beta_second), steps)
    offsets = (jnp.cumsum(tensor_rows) - tensor_rows).astype(jnp.int32)
    row_ids = jnp.arange(ROWS, dtype=jnp.int32)
    segment = (lax.optimization_barrier(jnp.sum((row_ids[:, None] >= offsets[None, :]).astype(jnp.int32), axis=1)) - 1).astype(jnp.int32)
    mask_rows = decay_mask.astype(jnp.float32)[segment]
    update = new_first / fix_first / (jnp.sqrt(new_second / fix_second) + adam_epsilon)
    update = update + decay_rate * mask_rows[:, None] * master
    weight_sq = jax.ops.segment_sum(lax.optimization_barrier(jnp.sum(master * master, axis=1)), segment, num_segments=TENSORS)
    update_sq = jax.ops.segment_sum(lax.optimization_barrier(jnp.sum(update * update, axis=1)), segment, num_segments=TENSORS)
    ratio = jnp.sqrt(weight_sq) / (jnp.sqrt(update_sq) + norm_epsilon)
    new_master = master - learn_rate * ratio[segment][:, None] * update
    return (new_master, new_first, new_second, new_master.astype(jnp.bfloat16))
```

```python
import functools

import jax
import jax.numpy as jnp
from jax import lax
from jax.experimental import pallas as pl
from jax.experimental.pallas import tpu as pltpu
from jax.sharding import PartitionSpec as P


beta_first = 0.9
beta_second = 0.999
adam_epsilon = 1e-06
decay_rate = 0.3
learn_rate = 0.3
norm_epsilon = 1e-06

LANES = 128
PIECES = 8
CHUNKS = 2
MIB = 1024 * 1024
f32, bf16 = jnp.float32, jnp.bfloat16
hbm = pl.BlockSpec(memory_space=pltpu.HBM)
vmem = pl.BlockSpec(memory_space=pltpu.VMEM)


def in_hbm(*arrays):
    return tuple(pltpu.with_memory_space_constraint(a, pltpu.HBM) for a in arrays)


def power(base, steps):
    return lax.fori_loop(0, steps, lambda _, p: p * base, jnp.float32(1.0))


def first_pass(step_count, rows_hbm, decay_hbm, master, moment_first, moment_second, gradients,
               kept_master, kept_first, kept_second, kept_update, member, sums,
               weight_rows, update_rows, mask_rows, tensor_rows, decay_mask, small_sems, sems):
    rows, cols = kept_master.shape
    piece = rows // PIECES
    small = []
    for a, (source, target) in enumerate(((rows_hbm, tensor_rows), (decay_hbm, decay_mask))):
        copy = pltpu.make_async_copy(source, target, small_sems.at[a])
        copy.start()
        small.append(copy)
    copies = []
    for p in range(PIECES):
        part = pl.ds(p * piece, piece)
        for a, (source, target) in enumerate((
            (master, kept_master), (moment_first, kept_first), (moment_second, kept_second), (gradients, kept_update),
        )):
            copy = pltpu.make_async_copy(source.at[part], target.at[part], sems.at[a, p])
            copy.start()
            copies.append(copy)
    for copy in small:
        copy.wait()

    steps = step_count[0]
    scale_first = 1.0 / (1.0 - jnp.full((8, LANES), power(jnp.float32(beta_first), steps)))
    scale_second = 1.0 / (1.0 - jnp.full((8, LANES), power(jnp.float32(beta_second), steps)))
    lane = lax.broadcasted_iota(jnp.int32, (8, LANES), 1)
    start = jnp.zeros((8, LANES), jnp.int32)
    end = jnp.zeros((8, LANES), jnp.int32)
    decay = jnp.zeros((8, LANES), f32)
    offset = jnp.int32(0)
    for k in range(tensor_rows.shape[0]):
        after = offset + tensor_rows[k]
        start = jnp.where(lane == k, offset, start)
        end = jnp.where(lane == k, after, end)
        decay = jnp.where(lane == k, decay_rate * decay_mask[k].astype(f32), decay)
        offset = after
    row = lax.axis_index("dp") * rows + lax.broadcasted_iota(jnp.int32, (8, LANES), 0)

    def belongs(i, carry):
        at = pl.ds(pl.multiple_of(i * 8, 8), 8)
        here = row + i * 8
        inside = jnp.where((here >= start) & (here < end), 1.0, 0.0)
        member[at] = inside
        mask_rows[at] = jnp.broadcast_to(jnp.sum(inside * decay, axis=1, keepdims=True), (8, LANES))
        return carry

    lax.fori_loop(0, rows // 8, belongs, 0, unroll=4)

    for p in range(PIECES):
        for copy in copies[4 * p:4 * p + 4]:
            copy.wait()

        def group(i, carry):
            at = pl.ds(pl.multiple_of(p * piece + i * 8, 8), 8)
            mask = mask_rows[at]
            weight = jnp.zeros((8, LANES), f32)
            total = jnp.zeros((8, LANES), f32)
            for t in range(cols // LANES):
                tile = (at, pl.ds(t * LANES, LANES))
                grad = kept_update[tile]
                value = kept_master[tile]
                new_first = beta_first * kept_first[tile] + (1.0 - beta_first) * grad
                new_second = beta_second * kept_second[tile] + (1.0 - beta_second) * grad * grad
                update = (new_first * scale_first) / (jnp.sqrt(new_second * scale_second) + adam_epsilon)
                update = update + mask * value
                kept_first[tile] = new_first
                kept_second[tile] = new_second
                kept_update[tile] = update
                weight = weight + value * value
                total = total + update * update
            weight_rows[at] = weight
            update_rows[at] = total
            return carry

        lax.fori_loop(0, piece // 8, group, 0)

    dims = (((0,), (0,)), ((), ()))
    dot = functools.partial(lax.dot_general, dimension_numbers=dims, precision=lax.Precision.HIGHEST, preferred_element_type=f32)
    per_weight = jnp.sum(dot(weight_rows[...], member[...]), axis=0, keepdims=True)
    per_update = jnp.sum(dot(update_rows[...], member[...]), axis=0, keepdims=True)
    both = jnp.concatenate([per_weight, per_update], axis=0)
    sums[...] = jnp.broadcast_to(both[None], sums.shape)


def rate_rows(sums, member):
    total = jnp.sum(sums[...], axis=0)
    ratio = jnp.sqrt(total[0:1]) / (jnp.sqrt(total[1:2]) + norm_epsilon)
    return jnp.sum(member * (learn_rate * ratio), axis=1, keepdims=True)


def round_pass(first, sums, member, kept_master, kept_update, chunk):
    part = pl.ds(first, chunk.shape[0])
    rate = rate_rows(sums, member[part])
    chunk[...] = (kept_master[part] - rate * kept_update[part]).astype(bf16)


def write_pass(sums, member, kept_master, kept_first, kept_second, kept_update,
               new_master, new_first, new_second, gathered, wide, narrow, sems):
    rows = kept_master.shape[0]
    one = pltpu.make_async_copy(kept_first, new_first, sems.at[0])
    two = pltpu.make_async_copy(kept_second, new_second, sems.at[1])
    one.start()
    two.start()
    wide[...] = kept_master[...] - rate_rows(sums, member[...]) * kept_update[...]
    narrow[...] = wide[...].astype(bf16)
    mine = pl.ds(pl.multiple_of(lax.axis_index("dp") * rows, rows), rows)
    three = pltpu.make_async_copy(wide, new_master, sems.at[2])
    four = pltpu.make_async_copy(narrow, gathered.at[mine], sems.at[3])
    three.start()
    four.start()
    for copy in (one, two, three, four):
        copy.wait()


def place_pass(chips, rows, items, before, *refs):
    pieces, (gathered, sems) = refs[:len(items)], refs[len(items):]
    me = lax.axis_index("dp")
    chip, core = me // 2, me % 2
    spot = jnp.where(chip % 2 == 0, chip // 2, chips - (chip + 1) // 2)
    copies = []
    for a, (step, swapped, first) in enumerate(items):
        at = (spot + chips - step) % chips
        source = jnp.where(2 * at < chips, 2 * at, 2 * (chips - at) - 1)
        owner = 2 * source + (1 - core if swapped else core)
        part = pl.ds(pl.multiple_of(owner * rows + first, 16), pieces[a].shape[0])
        copies.append(pltpu.make_async_copy(pieces[a], gathered.at[part], sems.at[a]))
        copies[-1].start()
    for copy in copies:
        copy.wait()


def place(chips, rows, items, gathered, *pieces):
    return pl.pallas_call(
        functools.partial(place_pass, chips, rows, items),
        out_shape=pltpu.HBM(gathered.shape, gathered.dtype),
        in_specs=[hbm] + [vmem] * len(items),
        out_specs=hbm,
        scratch_shapes=[pltpu.SemaphoreType.DMA((len(items),))],
        input_output_aliases={0: 0},
        compiler_params=pltpu.CompilerParams(vmem_limit_bytes=4 * MIB),
        name="place_pass",
    )(*in_hbm(gathered), *pieces)


def local(devices, dp, master, moment_first, moment_second, gradients, step_count, tensor_rows, decay_mask):
    rows, cols = master.shape
    kept = pltpu.VMEM((rows, cols), f32)
    small = [pltpu.SMEM(a.shape, a.dtype) for a in (tensor_rows, decay_mask)]

    kept_master, kept_first, kept_second, kept_update, member, sums = pl.pallas_call(
        first_pass,
        out_shape=(kept, kept, kept, kept, pltpu.VMEM((rows, LANES), f32), jax.ShapeDtypeStruct((devices, 2, LANES), f32)),
        in_specs=[pl.BlockSpec(memory_space=pltpu.SMEM)] + [hbm] * 6,
        out_specs=(vmem,) * 6,
        scratch_shapes=[pltpu.VMEM((rows, LANES), f32)] * 3 + small
        + [pltpu.SemaphoreType.DMA((2,)), pltpu.SemaphoreType.DMA((4, PIECES))],
        compiler_params=pltpu.CompilerParams(vmem_limit_bytes=4 * MIB),
        name="first_pass",
    )(step_count, *in_hbm(tensor_rows, decay_mask, master, moment_first, moment_second, gradients))

    sums = lax.all_to_all(sums, ("dp", "mp"), 0, 0, tiled=True)

    size = rows // CHUNKS
    pieces = []
    for i in range(CHUNKS):
        pieces.append(pl.pallas_call(
            functools.partial(round_pass, i * size),
            out_shape=pltpu.VMEM((size, cols), bf16),
            in_specs=[vmem] * 4,
            out_specs=vmem,
            compiler_params=pltpu.CompilerParams(vmem_limit_bytes=4 * MIB),
            name="round_pass",
        )(sums, member, kept_master, kept_update))

    new_master, new_first, new_second, gathered = pl.pallas_call(
        write_pass,
        out_shape=(jax.ShapeDtypeStruct((rows, cols), f32),) * 3 + (pltpu.HBM((dp * rows, cols), bf16),),
        in_specs=[vmem] * 6,
        out_specs=(hbm,) * 4,
        scratch_shapes=[pltpu.VMEM((rows, cols), f32), pltpu.VMEM((rows, cols), bf16), pltpu.SemaphoreType.DMA((4,))],
        compiler_params=pltpu.CompilerParams(vmem_limit_bytes=8 * MIB),
        name="write_pass",
    )(sums, member, kept_master, kept_first, kept_second, kept_update)

    chips = dp // 2
    order = [2 * p if 2 * p < chips else 2 * (chips - p) - 1 for p in range(chips)]
    ring = [(2 * order[p] + c, 2 * order[(p + 1) % chips] + c) for p in range(chips) for c in range(2)]
    partner = [(d, d ^ 1) for d in range(dp)]
    others = []
    for k in range(chips):
        for i in range(CHUNKS):
            piece, first = pieces[i], i * size
            if k < chips - 1:
                pieces[i] = lax.ppermute(piece, "dp", ring)
            other = lax.ppermute(piece, "dp", partner)
            if k == 0:
                others.append(other)
                if i == CHUNKS - 1:
                    gathered = place(chips, rows, tuple((0, True, j * size) for j in range(CHUNKS)), gathered, *others)
            elif k == chips - 1 and i == CHUNKS - 1:
                gathered = place(chips, rows, ((k, False, first),), gathered, piece)
                gathered = place(chips, rows, ((k, True, first),), gathered, other)
            else:
                gathered = place(chips, rows, ((k, False, first), (k, True, first)), gathered, piece, other)
    return new_master, new_first, new_second, gathered


def solution(mesh):
    placed = (P("dp", "mp"), P("dp", "mp"), P("dp", "mp"), P("dp", "mp"), P(), P(), P())
    body = functools.partial(local, mesh.size, mesh.shape["dp"])

    return jax.shard_map(
        body,
        mesh=mesh,
        in_specs=placed,
        out_specs=(P("dp", "mp"), P("dp", "mp"), P("dp", "mp"), P(None, "mp")),
        check_vma=False,
    )
```

```python
import functools

import jax
import jax.numpy as jnp
from jax import lax
from jax.experimental import pallas as pl
from jax.experimental.pallas import tpu as pltpu
from jax.sharding import PartitionSpec as P


beta_first = 0.9
beta_second = 0.999
adam_epsilon = 1e-06
decay_rate = 0.3
learn_rate = 0.3
norm_epsilon = 1e-06

LANES = 128
TILE = 8
PIECE = 64
SHARES = (3, 1)
CHUNKS = len(SHARES)
MIB = 1024 * 1024
f32, bf16 = jnp.float32, jnp.bfloat16
hbm = pl.BlockSpec(memory_space=pltpu.HBM)
vmem = pl.BlockSpec(memory_space=pltpu.VMEM)


def in_hbm(*arrays):
    return tuple(pltpu.with_memory_space_constraint(a, pltpu.HBM) for a in arrays)


def power(base, steps):
    return lax.fori_loop(0, steps, lambda _, p: p * base, jnp.float32(1.0))


def piece_sizes(rows):
    return [PIECE] * (rows // PIECE - 1) + [PIECE // 2] * 2


def first_pass(step_count, rows_hbm, decay_hbm, master, moment_first, moment_second, gradients,
               kept_master, kept_first, kept_second, kept_grad, kept_update, member, sums,
               weight_rows, update_rows, mask_rows, tensor_rows, decay_mask, small_sems, sems):
    rows, cols = kept_master.shape
    small = []
    for a, (source, target) in enumerate(((rows_hbm, tensor_rows), (decay_hbm, decay_mask))):
        copy = pltpu.make_async_copy(source, target, small_sems.at[a])
        copy.start()
        small.append(copy)
    pieces, begin = [], 0
    for p, size in enumerate(piece_sizes(rows)):
        part = pl.ds(begin, size)
        copies = []
        for a, (source, target) in enumerate((
            (master, kept_master), (moment_first, kept_first), (moment_second, kept_second), (gradients, kept_grad),
        )):
            copies.append(pltpu.make_async_copy(source.at[part], target.at[part], sems.at[a, p]))
            copies[-1].start()
        pieces.append((begin, size, copies))
        begin += size
    for copy in small:
        copy.wait()

    steps = step_count[0]
    scale_first = 1.0 / (1.0 - jnp.full((TILE, LANES), power(jnp.float32(beta_first), steps)))
    scale_second = 1.0 / (1.0 - jnp.full((TILE, LANES), power(jnp.float32(beta_second), steps)))
    old_first, old_second = beta_first * scale_first, beta_second * scale_second
    add_first, add_second = (1.0 - beta_first) * scale_first, (1.0 - beta_second) * scale_second
    lane = lax.broadcasted_iota(jnp.int32, (TILE, LANES), 1)
    start = jnp.zeros((TILE, LANES), jnp.int32)
    end = jnp.zeros((TILE, LANES), jnp.int32)
    decay = jnp.zeros((TILE, LANES), f32)
    offset = jnp.int32(0)
    for k in range(tensor_rows.shape[0]):
        after = offset + tensor_rows[k]
        start = jnp.where(lane == k, offset, start)
        end = jnp.where(lane == k, after, end)
        decay = jnp.where(lane == k, decay_rate * decay_mask[k].astype(f32), decay)
        offset = after
    row = lax.axis_index("dp") * rows + lax.broadcasted_iota(jnp.int32, (TILE, LANES), 0)

    def belongs(i, carry):
        at = pl.ds(pl.multiple_of(i * TILE, TILE), TILE)
        here = row + i * TILE
        inside = jnp.where((here >= start) & (here < end), 1.0, 0.0)
        member[at] = inside
        mask_rows[at] = jnp.broadcast_to(jnp.sum(inside * decay, axis=1, keepdims=True), (TILE, LANES))
        return carry

    per_weight = jnp.zeros((TILE, LANES), f32)
    per_update = jnp.zeros((TILE, LANES), f32)
    for begin, size, copies in pieces:
        lax.fori_loop(begin // TILE, (begin + size) // TILE, belongs, 0, unroll=True)
        for copy in copies:
            copy.wait()

        def group(i, carry):
            at = pl.ds(pl.multiple_of(begin + i * TILE, TILE), TILE)
            mask = mask_rows[at]
            weight = jnp.zeros((TILE, LANES), f32)
            total = jnp.zeros((TILE, LANES), f32)
            for t in range(cols // LANES):
                tile = (at, pl.ds(t * LANES, LANES))
                grad = kept_grad[tile]
                value = kept_master[tile]
                top = old_first * kept_first[tile] + add_first * grad
                square = old_second * kept_second[tile] + add_second * grad * grad
                update = top * pl.reciprocal(square * lax.rsqrt(square) + adam_epsilon) + mask * value
                kept_update[tile] = update
                weight = weight + value * value
                total = total + update * update
            weight_rows[at] = weight
            update_rows[at] = total
            return carry

        lax.fori_loop(0, size // TILE, group, 0, unroll=4)
        for i in range(size // TILE):
            at = pl.ds(begin + i * TILE, TILE)
            inside = member[at]
            per_weight = per_weight + inside * jnp.sum(weight_rows[at], axis=1, keepdims=True)
            per_update = per_update + inside * jnp.sum(update_rows[at], axis=1, keepdims=True)

    both = jnp.concatenate(
        [jnp.sum(per_weight, axis=0, keepdims=True), jnp.sum(per_update, axis=0, keepdims=True)], axis=0
    )
    sums[...] = jnp.broadcast_to(both[None], sums.shape)


def rate_rows(sums, member):
    total = jnp.sum(sums[...], axis=0)
    ratio = jnp.sqrt(total[0:1]) / (jnp.sqrt(total[1:2]) + norm_epsilon)
    return jnp.sum(member * (learn_rate * ratio), axis=1, keepdims=True)


def round_pass(first, sums, member, kept_master, kept_update, chunk):
    part = pl.ds(first, chunk.shape[0])
    rate = rate_rows(sums, member[part])
    chunk[...] = (kept_master[part] - rate * kept_update[part]).astype(bf16)


def write_pass(sums, member, kept_master, kept_first, kept_second, kept_grad, kept_update,
               new_master, new_first, new_second, gathered, one, two, three, four, sems):
    rows = kept_master.shape[0]
    mine = pl.ds(pl.multiple_of(lax.axis_index("dp") * rows, rows), rows)
    copies = [
        pltpu.make_async_copy(source, target, sems.at[a]) for a, (source, target) in enumerate(
            ((one, new_first), (two, new_second), (three, new_master), (four, gathered.at[mine])))
    ]
    grad = kept_grad[...]
    one[...] = beta_first * kept_first[...] + (1.0 - beta_first) * grad
    copies[0].start()
    two[...] = beta_second * kept_second[...] + (1.0 - beta_second) * grad * grad
    copies[1].start()
    three[...] = kept_master[...] - rate_rows(sums, member[...]) * kept_update[...]
    copies[2].start()
    four[...] = three[...].astype(bf16)
    copies[3].start()
    for copy in copies:
        copy.wait()


def place_pass(chips, rows, items, before, *refs):
    pieces, (gathered, sems) = refs[:len(items)], refs[len(items):]
    me = lax.axis_index("dp")
    chip, core = me // 2, me % 2
    spot = jnp.where(chip % 2 == 0, chip // 2, chips - (chip + 1) // 2)
    copies = []
    for a, (step, swapped, first) in enumerate(items):
        at = (spot + chips - step) % chips
        source = jnp.where(2 * at < chips, 2 * at, 2 * (chips - at) - 1)
        owner = 2 * source + (1 - core if swapped else core)
        part = pl.ds(pl.multiple_of(owner * rows + first, 16), pieces[a].shape[0])
        copies.append(pltpu.make_async_copy(pieces[a], gathered.at[part], sems.at[a]))
        copies[-1].start()
    for copy in copies:
        copy.wait()


def place(chips, rows, items, gathered, *pieces):
    return pl.pallas_call(
        functools.partial(place_pass, chips, rows, items),
        out_shape=pltpu.HBM(gathered.shape, gathered.dtype),
        in_specs=[hbm] + [vmem] * len(items),
        out_specs=hbm,
        scratch_shapes=[pltpu.SemaphoreType.DMA((len(items),))],
        input_output_aliases={0: 0},
        compiler_params=pltpu.CompilerParams(vmem_limit_bytes=4 * MIB),
        name="place_pass",
    )(*in_hbm(gathered), *pieces)


def local(devices, dp, master, moment_first, moment_second, gradients, step_count, tensor_rows, decay_mask):
    rows, cols = master.shape
    kept = pltpu.VMEM((rows, cols), f32)
    small = [pltpu.SMEM(a.shape, a.dtype) for a in (tensor_rows, decay_mask)]

    kept_master, kept_first, kept_second, kept_grad, kept_update, member, sums = pl.pallas_call(
        first_pass,
        out_shape=(kept,) * 5 + (pltpu.VMEM((rows, LANES), f32), jax.ShapeDtypeStruct((devices, 2, LANES), f32)),
        in_specs=[pl.BlockSpec(memory_space=pltpu.SMEM)] + [hbm] * 6,
        out_specs=(vmem,) * 7,
        scratch_shapes=[pltpu.VMEM((rows, LANES), f32)] * 3 + small
        + [pltpu.SemaphoreType.DMA((2,)), pltpu.SemaphoreType.DMA((4, len(piece_sizes(rows))))],
        compiler_params=pltpu.CompilerParams(vmem_limit_bytes=4 * MIB),
        name="first_pass",
    )(step_count, *in_hbm(tensor_rows, decay_mask, master, moment_first, moment_second, gradients))

    sums = lax.all_to_all(sums, ("dp", "mp"), 0, 0, tiled=True)

    sizes = [rows * share // sum(SHARES) for share in SHARES]
    firsts = [sum(sizes[:i]) for i in range(CHUNKS)]
    pieces = []
    for i in range(CHUNKS):
        pieces.append(pl.pallas_call(
            functools.partial(round_pass, firsts[i]),
            out_shape=pltpu.VMEM((sizes[i], cols), bf16),
            in_specs=[vmem] * 4,
            out_specs=vmem,
            compiler_params=pltpu.CompilerParams(vmem_limit_bytes=4 * MIB),
            name="round_pass",
        )(sums, member, kept_master, kept_update))

    new_master, new_first, new_second, gathered = pl.pallas_call(
        write_pass,
        out_shape=(jax.ShapeDtypeStruct((rows, cols), f32),) * 3 + (pltpu.HBM((dp * rows, cols), bf16),),
        in_specs=[vmem] * 7,
        out_specs=(hbm,) * 4,
        scratch_shapes=[pltpu.VMEM((rows, cols), f32)] * 3 + [pltpu.VMEM((rows, cols), bf16), pltpu.SemaphoreType.DMA((4,))],
        compiler_params=pltpu.CompilerParams(vmem_limit_bytes=24 * MIB),
        name="write_pass",
    )(sums, member, kept_master, kept_first, kept_second, kept_grad, kept_update)

    chips = dp // 2
    order = [2 * p if 2 * p < chips else 2 * (chips - p) - 1 for p in range(chips)]
    ring = [(2 * order[p] + c, 2 * order[(p + 1) % chips] + c) for p in range(chips) for c in range(2)]
    partner = [(d, d ^ 1) for d in range(dp)]
    others = []
    for k in range(chips):
        for i in range(CHUNKS):
            piece, first = pieces[i], firsts[i]
            if k < chips - 1:
                pieces[i] = lax.ppermute(piece, "dp", ring)
            other = lax.ppermute(piece, "dp", partner)
            if k == 0:
                others.append(other)
                if i == CHUNKS - 1:
                    gathered = place(chips, rows, tuple((0, True, first) for first in firsts), gathered, *others)
            elif k == chips - 1 and i == CHUNKS - 1:
                gathered = place(chips, rows, ((k, False, first),), gathered, piece)
                gathered = place(chips, rows, ((k, True, first),), gathered, other)
            else:
                gathered = place(chips, rows, ((k, False, first), (k, True, first)), gathered, piece, other)
    return new_master, new_first, new_second, gathered


def solution(mesh):
    placed = (P("dp", "mp"), P("dp", "mp"), P("dp", "mp"), P("dp", "mp"), P(), P(), P())
    body = functools.partial(local, mesh.size, mesh.shape["dp"])

    return jax.shard_map(
        body,
        mesh=mesh,
        in_specs=placed,
        out_specs=(P("dp", "mp"), P("dp", "mp"), P("dp", "mp"), P(None, "mp")),
        check_vma=False,
    )
```

```python
import functools

import jax
import jax.numpy as jnp
from jax import lax
from jax.experimental import pallas as pl
from jax.experimental.pallas import tpu as pltpu
from jax.sharding import PartitionSpec as P


beta_first = 0.9
beta_second = 0.999
adam_epsilon = 1e-06
decay_rate = 0.3
learn_rate = 0.3
norm_epsilon = 1e-06

LANES = 128
TILE = 8
PIECE = 64
SHARES = (3, 1)
CHUNKS = len(SHARES)
EARLY = 16
MIB = 1024 * 1024
f32, bf16 = jnp.float32, jnp.bfloat16
hbm = pl.BlockSpec(memory_space=pltpu.HBM)
vmem = pl.BlockSpec(memory_space=pltpu.VMEM)


def in_hbm(*arrays):
    return tuple(pltpu.with_memory_space_constraint(a, pltpu.HBM) for a in arrays)


def power(base, steps):
    return lax.fori_loop(0, steps, lambda _, p: p * base, jnp.float32(1.0))


def piece_sizes(rows):
    return [PIECE] * (rows // PIECE - 1) + [PIECE // 2] * 2


def first_pass(step_count, rows_hbm, decay_hbm, master, moment_first, moment_second, gradients,
               kept_master, kept_first, kept_second, kept_grad, kept_update, member, bounds, pair, sums,
               weight_rows, update_rows, mask_rows, tensor_rows, decay_mask, small_sems, sems):
    rows, cols = kept_master.shape
    small = []
    for a, (source, target) in enumerate(((rows_hbm, tensor_rows), (decay_hbm, decay_mask))):
        copy = pltpu.make_async_copy(source, target, small_sems.at[a])
        copy.start()
        small.append(copy)
    pieces, begin = [], 0
    for p, size in enumerate(piece_sizes(rows)):
        part = pl.ds(begin, size)
        copies = []
        for a, (source, target) in enumerate((
            (master, kept_master), (moment_first, kept_first), (moment_second, kept_second), (gradients, kept_grad),
        )):
            copies.append(pltpu.make_async_copy(source.at[part], target.at[part], sems.at[a, p]))
            copies[-1].start()
        pieces.append((begin, size, copies))
        begin += size
    for copy in small:
        copy.wait()

    steps = step_count[0]
    scale_first = 1.0 / (1.0 - jnp.full((TILE, LANES), power(jnp.float32(beta_first), steps)))
    scale_second = 1.0 / (1.0 - jnp.full((TILE, LANES), power(jnp.float32(beta_second), steps)))
    old_first, old_second = beta_first * scale_first, beta_second * scale_second
    add_first, add_second = (1.0 - beta_first) * scale_first, (1.0 - beta_second) * scale_second
    lane = lax.broadcasted_iota(jnp.int32, (TILE, LANES), 1)
    start = jnp.zeros((TILE, LANES), jnp.int32)
    end = jnp.zeros((TILE, LANES), jnp.int32)
    decay = jnp.zeros((TILE, LANES), f32)
    offset = jnp.int32(0)
    for k in range(tensor_rows.shape[0]):
        after = offset + tensor_rows[k]
        start = jnp.where(lane == k, offset, start)
        end = jnp.where(lane == k, after, end)
        decay = jnp.where(lane == k, decay_rate * decay_mask[k].astype(f32), decay)
        offset = after
    bounds[0] = start
    bounds[1] = end
    row = lax.axis_index("dp") * rows + lax.broadcasted_iota(jnp.int32, (TILE, LANES), 0)

    def belongs(i, carry):
        at = pl.ds(pl.multiple_of(i * TILE, TILE), TILE)
        here = row + i * TILE
        inside = jnp.where((here >= start) & (here < end), 1.0, 0.0)
        member[at] = inside
        mask_rows[at] = jnp.broadcast_to(jnp.sum(inside * decay, axis=1, keepdims=True), (TILE, LANES))
        return carry

    per_weight = jnp.zeros((TILE, LANES), f32)
    per_update = jnp.zeros((TILE, LANES), f32)
    for begin, size, copies in pieces:
        lax.fori_loop(begin // TILE, (begin + size) // TILE, belongs, 0, unroll=True)
        for copy in copies:
            copy.wait()

        def group(i, carry):
            at = pl.ds(pl.multiple_of(begin + i * TILE, TILE), TILE)
            mask = mask_rows[at]
            weight = jnp.zeros((TILE, LANES), f32)
            total = jnp.zeros((TILE, LANES), f32)
            for t in range(cols // LANES):
                tile = (at, pl.ds(t * LANES, LANES))
                grad = kept_grad[tile]
                value = kept_master[tile]
                top = old_first * kept_first[tile] + add_first * grad
                square = old_second * kept_second[tile] + add_second * grad * grad
                update = top * pl.reciprocal(square * lax.rsqrt(square) + adam_epsilon) + mask * value
                kept_update[tile] = update
                weight = weight + value * value
                total = total + update * update
            weight_rows[at] = weight
            update_rows[at] = total
            return carry

        lax.fori_loop(0, size // TILE, group, 0, unroll=4)
        for i in range(size // TILE):
            at = pl.ds(begin + i * TILE, TILE)
            inside = member[at]
            per_weight = per_weight + inside * jnp.sum(weight_rows[at], axis=1, keepdims=True)
            per_update = per_update + inside * jnp.sum(update_rows[at], axis=1, keepdims=True)

    early = pair.shape[1]
    pair[0] = kept_master[pl.ds(rows - early, early)]
    pair[1] = kept_update[pl.ds(rows - early, early)]
    both = jnp.concatenate(
        [jnp.sum(per_weight, axis=0, keepdims=True), jnp.sum(per_update, axis=0, keepdims=True)], axis=0
    )
    sums[...] = jnp.broadcast_to(both[None], sums.shape)


def rate_rows(sums, member):
    total = jnp.sum(sums[...], axis=0)
    ratio = jnp.sqrt(total[0:1]) / (jnp.sqrt(total[1:2]) + norm_epsilon)
    return jnp.sum(member * (learn_rate * ratio), axis=1, keepdims=True)


def round_pass(first, sums, member, kept_master, kept_update, *chunks):
    part = pl.ds(first, chunks[0].shape[0])
    rate = rate_rows(sums, member[part])
    values = (kept_master[part] - rate * kept_update[part]).astype(bf16)
    for chunk in chunks:
        chunk[...] = values[:chunk.shape[0]]


def ring_owner(chips, step):
    chip = lax.axis_index("dp") // 2
    spot = jnp.where(chip % 2 == 0, chip // 2, chips - (chip + 1) // 2)
    at = (spot + chips - step) % chips
    return jnp.where(2 * at < chips, 2 * at, 2 * (chips - at) - 1)


def merge_pass(chips, rows, sums, bounds, short, pair, chunk):
    early = pair.shape[1]
    owner = 2 * ring_owner(chips, 1) + lax.axis_index("dp") % 2
    row = owner * rows + rows - early + lax.broadcasted_iota(jnp.int32, (early, LANES), 0)
    member = jnp.where((row >= bounds[0, 0:1]) & (row < bounds[1, 0:1]), 1.0, 0.0)
    chunk[pl.ds(0, short.shape[0])] = short[...]
    chunk[pl.ds(short.shape[0], early)] = (pair[0] - rate_rows(sums, member) * pair[1]).astype(bf16)


def write_pass(sums, member, kept_master, kept_first, kept_second, kept_grad, kept_update,
               new_master, new_first, new_second, gathered, one, two, three, four, sems):
    rows = kept_master.shape[0]
    mine = pl.ds(pl.multiple_of(lax.axis_index("dp") * rows, rows), rows)
    copies = [
        pltpu.make_async_copy(source, target, sems.at[a]) for a, (source, target) in enumerate(
            ((one, new_first), (two, new_second), (three, new_master), (four, gathered.at[mine])))
    ]
    grad = kept_grad[...]
    one[...] = beta_first * kept_first[...] + (1.0 - beta_first) * grad
    copies[0].start()
    two[...] = beta_second * kept_second[...] + (1.0 - beta_second) * grad * grad
    copies[1].start()
    three[...] = kept_master[...] - rate_rows(sums, member[...]) * kept_update[...]
    copies[2].start()
    four[...] = three[...].astype(bf16)
    copies[3].start()
    for copy in copies:
        copy.wait()


def place_pass(chips, rows, items, before, *refs):
    pieces, (gathered, sems) = refs[:len(items)], refs[len(items):]
    core = lax.axis_index("dp") % 2
    copies = []
    for a, (step, swapped, first) in enumerate(items):
        owner = 2 * ring_owner(chips, step) + (1 - core if swapped else core)
        part = pl.ds(pl.multiple_of(owner * rows + first, 16), pieces[a].shape[0])
        copies.append(pltpu.make_async_copy(pieces[a], gathered.at[part], sems.at[a]))
        copies[-1].start()
    for copy in copies:
        copy.wait()


def place(chips, rows, items, gathered, *pieces):
    return pl.pallas_call(
        functools.partial(place_pass, chips, rows, items),
        out_shape=pltpu.HBM(gathered.shape, gathered.dtype),
        in_specs=[hbm] + [vmem] * len(items),
        out_specs=hbm,
        scratch_shapes=[pltpu.SemaphoreType.DMA((len(items),))],
        input_output_aliases={0: 0},
        compiler_params=pltpu.CompilerParams(vmem_limit_bytes=4 * MIB),
        name="place_pass",
    )(*in_hbm(gathered), *pieces)


def local(devices, dp, master, moment_first, moment_second, gradients, step_count, tensor_rows, decay_mask):
    rows, cols = master.shape
    kept = pltpu.VMEM((rows, cols), f32)
    early = rows // EARLY
    chips = dp // 2
    order = [2 * p if 2 * p < chips else 2 * (chips - p) - 1 for p in range(chips)]
    ring = [(2 * order[p] + c, 2 * order[(p + 1) % chips] + c) for p in range(chips) for c in range(2)]
    partner = [(d, d ^ 1) for d in range(dp)]
    small = [pltpu.SMEM(a.shape, a.dtype) for a in (tensor_rows, decay_mask)]

    kept_master, kept_first, kept_second, kept_grad, kept_update, member, bounds, pair, sums = pl.pallas_call(
        first_pass,
        out_shape=(kept,) * 5 + (
            pltpu.VMEM((rows, LANES), f32), pltpu.VMEM((2, TILE, LANES), jnp.int32), pltpu.VMEM((2, early, cols), f32),
            jax.ShapeDtypeStruct((devices, 2, LANES), f32)),
        in_specs=[pl.BlockSpec(memory_space=pltpu.SMEM)] + [hbm] * 6,
        out_specs=(vmem,) * 9,
        scratch_shapes=[pltpu.VMEM((rows, LANES), f32)] * 3 + small
        + [pltpu.SemaphoreType.DMA((2,)), pltpu.SemaphoreType.DMA((4, len(piece_sizes(rows))))],
        compiler_params=pltpu.CompilerParams(vmem_limit_bytes=4 * MIB),
        name="first_pass",
    )(step_count, *in_hbm(tensor_rows, decay_mask, master, moment_first, moment_second, gradients))

    pair = lax.ppermute(pair, "dp", ring)
    sums = lax.all_to_all(sums, ("dp", "mp"), 0, 0, tiled=True)

    sizes = [rows * share // sum(SHARES) for share in SHARES]
    firsts = [sum(sizes[:i]) for i in range(CHUNKS)]
    pieces = []
    for i in range(CHUNKS):
        shapes = (sizes[i],) if i < CHUNKS - 1 else (sizes[i], sizes[i] - early)
        pieces.append(pl.pallas_call(
            functools.partial(round_pass, firsts[i]),
            out_shape=tuple(pltpu.VMEM((size, cols), bf16) for size in shapes),
            in_specs=[vmem] * 4,
            out_specs=(vmem,) * len(shapes),
            compiler_params=pltpu.CompilerParams(vmem_limit_bytes=4 * MIB),
            name="round_pass",
        )(sums, member, kept_master, kept_update))

    new_master, new_first, new_second, gathered = pl.pallas_call(
        write_pass,
        out_shape=(jax.ShapeDtypeStruct((rows, cols), f32),) * 3 + (pltpu.HBM((dp * rows, cols), bf16),),
        in_specs=[vmem] * 7,
        out_specs=(hbm,) * 4,
        scratch_shapes=[pltpu.VMEM((rows, cols), f32)] * 3 + [pltpu.VMEM((rows, cols), bf16), pltpu.SemaphoreType.DMA((4,))],
        compiler_params=pltpu.CompilerParams(vmem_limit_bytes=24 * MIB),
        name="write_pass",
    )(sums, member, kept_master, kept_first, kept_second, kept_grad, kept_update)

    short = pieces[-1][1]
    pieces = [piece[0] for piece in pieces]
    others = []
    for k in range(chips):
        for i in range(CHUNKS):
            piece, first = pieces[i], firsts[i]
            if k < chips - 1:
                pieces[i] = lax.ppermute(short if (k, i) == (0, CHUNKS - 1) else piece, "dp", ring)
                if (k, i) == (0, CHUNKS - 1):
                    pieces[i] = pl.pallas_call(
                        functools.partial(merge_pass, chips, rows),
                        out_shape=pltpu.VMEM((sizes[i], cols), bf16),
                        in_specs=[vmem] * 4,
                        out_specs=vmem,
                        compiler_params=pltpu.CompilerParams(vmem_limit_bytes=4 * MIB),
                        name="merge_pass",
                    )(sums, bounds, pieces[i], pair)
            other = lax.ppermute(piece, "dp", partner)
            if k == 0:
                others.append(other)
                if i == CHUNKS - 1:
                    gathered = place(chips, rows, tuple((0, True, first) for first in firsts), gathered, *others)
            elif k == chips - 1 and i == CHUNKS - 1:
                gathered = place(chips, rows, ((k, False, first),), gathered, piece)
                gathered = place(chips, rows, ((k, True, first),), gathered, other)
            else:
                gathered = place(chips, rows, ((k, False, first), (k, True, first)), gathered, piece, other)
    return new_master, new_first, new_second, gathered


def solution(mesh):
    placed = (P("dp", "mp"), P("dp", "mp"), P("dp", "mp"), P("dp", "mp"), P(), P(), P())
    body = functools.partial(local, mesh.size, mesh.shape["dp"])

    return jax.shard_map(
        body,
        mesh=mesh,
        in_specs=placed,
        out_specs=(P("dp", "mp"), P("dp", "mp"), P("dp", "mp"), P(None, "mp")),
        check_vma=False,
    )
```

```python
import functools

import jax
import jax.numpy as jnp
from jax import lax
from jax.experimental import pallas as pl
from jax.experimental.pallas import tpu as pltpu
from jax.sharding import PartitionSpec as P


beta_first = 0.9
beta_second = 0.999
adam_epsilon = 1e-06
decay_rate = 0.3
learn_rate = 0.3
norm_epsilon = 1e-06

LANES = 128
TILE = 8
PIECE = 128
SHARES = (1, 2, 1)
CHUNKS = len(SHARES)
EARLY = 16
MIB = 1024 * 1024
f32, bf16 = jnp.float32, jnp.bfloat16
hbm = pl.BlockSpec(memory_space=pltpu.HBM)
vmem = pl.BlockSpec(memory_space=pltpu.VMEM)


def in_hbm(*arrays):
    return tuple(pltpu.with_memory_space_constraint(a, pltpu.HBM) for a in arrays)


def power(base, steps):
    return lax.fori_loop(0, steps, lambda _, p: p * base, jnp.float32(1.0))


def piece_sizes(rows):
    return [PIECE] * (rows // PIECE - 1) + [PIECE // 2] * 2


def first_pass(step_count, rows_hbm, decay_hbm, master, moment_first, moment_second, gradients,
               kept_master, kept_first, kept_second, kept_grad, kept_update, member, bounds, pair, sums,
               weight_rows, update_rows, mask_rows, tensor_rows, decay_mask, small_sems, sems):
    rows, cols = kept_master.shape
    small = []
    for a, (source, target) in enumerate(((rows_hbm, tensor_rows), (decay_hbm, decay_mask))):
        copy = pltpu.make_async_copy(source, target, small_sems.at[a])
        copy.start()
        small.append(copy)
    pieces, begin = [], 0
    for p, size in enumerate(piece_sizes(rows)):
        part = pl.ds(begin, size)
        copies = []
        for a, (source, target) in enumerate((
            (master, kept_master), (moment_first, kept_first), (moment_second, kept_second), (gradients, kept_grad),
        )):
            copies.append(pltpu.make_async_copy(source.at[part], target.at[part], sems.at[a, p]))
            copies[-1].start()
        pieces.append((begin, size, copies))
        begin += size
    for copy in small:
        copy.wait()

    steps = step_count[0]
    scale_first = 1.0 / (1.0 - jnp.full((TILE, LANES), power(jnp.float32(beta_first), steps)))
    scale_second = 1.0 / (1.0 - jnp.full((TILE, LANES), power(jnp.float32(beta_second), steps)))
    old_first, old_second = beta_first * scale_first, beta_second * scale_second
    add_first, add_second = (1.0 - beta_first) * scale_first, (1.0 - beta_second) * scale_second
    lane = lax.broadcasted_iota(jnp.int32, (TILE, LANES), 1)
    start = jnp.zeros((TILE, LANES), jnp.int32)
    end = jnp.zeros((TILE, LANES), jnp.int32)
    decay = jnp.zeros((TILE, LANES), f32)
    offset = jnp.int32(0)
    for k in range(tensor_rows.shape[0]):
        after = offset + tensor_rows[k]
        start = jnp.where(lane == k, offset, start)
        end = jnp.where(lane == k, after, end)
        decay = jnp.where(lane == k, decay_rate * decay_mask[k].astype(f32), decay)
        offset = after
    bounds[0] = start
    bounds[1] = end
    row = lax.axis_index("dp") * rows + lax.broadcasted_iota(jnp.int32, (TILE, LANES), 0)

    def belongs(i, carry):
        at = pl.ds(pl.multiple_of(i * TILE, TILE), TILE)
        here = row + i * TILE
        inside = jnp.where((here >= start) & (here < end), 1.0, 0.0)
        member[at] = inside
        mask_rows[at] = jnp.broadcast_to(jnp.sum(inside * decay, axis=1, keepdims=True), (TILE, LANES))
        return carry

    per_weight = jnp.zeros((TILE, LANES), f32)
    per_update = jnp.zeros((TILE, LANES), f32)
    for begin, size, copies in pieces:
        lax.fori_loop(begin // TILE, (begin + size) // TILE, belongs, 0, unroll=True)
        for copy in copies:
            copy.wait()

        def group(i, carry):
            at = pl.ds(pl.multiple_of(begin + i * TILE, TILE), TILE)
            mask = mask_rows[at]
            weight = jnp.zeros((TILE, LANES), f32)
            total = jnp.zeros((TILE, LANES), f32)
            for t in range(cols // LANES):
                tile = (at, pl.ds(t * LANES, LANES))
                grad = kept_grad[tile]
                value = kept_master[tile]
                top = old_first * kept_first[tile] + add_first * grad
                square = old_second * kept_second[tile] + add_second * grad * grad
                update = top * pl.reciprocal(square * lax.rsqrt(square) + adam_epsilon) + mask * value
                kept_update[tile] = update
                weight = weight + value * value
                total = total + update * update
            weight_rows[at] = weight
            update_rows[at] = total
            return carry

        lax.fori_loop(0, size // TILE, group, 0, unroll=8)
        for i in range(size // TILE):
            at = pl.ds(begin + i * TILE, TILE)
            inside = member[at]
            per_weight = per_weight + inside * jnp.sum(weight_rows[at], axis=1, keepdims=True)
            per_update = per_update + inside * jnp.sum(update_rows[at], axis=1, keepdims=True)

    early = pair.shape[1]
    pair[0] = kept_master[pl.ds(rows - early, early)]
    pair[1] = kept_update[pl.ds(rows - early, early)]
    both = jnp.concatenate(
        [jnp.sum(per_weight, axis=0, keepdims=True), jnp.sum(per_update, axis=0, keepdims=True)], axis=0
    )
    sums[...] = jnp.broadcast_to(both[None], sums.shape)


def rate_rows(sums, member):
    total = jnp.sum(sums[...], axis=0)
    ratio = jnp.sqrt(total[0:1]) / (jnp.sqrt(total[1:2]) + norm_epsilon)
    return jnp.sum(member * (learn_rate * ratio), axis=1, keepdims=True)


def round_pass(first, sums, member, kept_master, kept_update, *chunks):
    part = pl.ds(first, chunks[0].shape[0])
    rate = rate_rows(sums, member[part])
    values = (kept_master[part] - rate * kept_update[part]).astype(bf16)
    for chunk in chunks:
        chunk[...] = values[:chunk.shape[0]]


def ring_owner(chips, step):
    chip = lax.axis_index("dp") // 2
    spot = jnp.where(chip % 2 == 0, chip // 2, chips - (chip + 1) // 2)
    at = (spot + chips - step) % chips
    return jnp.where(2 * at < chips, 2 * at, 2 * (chips - at) - 1)


def merge_pass(chips, rows, sums, bounds, short, pair, chunk):
    early = pair.shape[1]
    owner = 2 * ring_owner(chips, 1) + lax.axis_index("dp") % 2
    row = owner * rows + rows - early + lax.broadcasted_iota(jnp.int32, (early, LANES), 0)
    member = jnp.where((row >= bounds[0, 0:1]) & (row < bounds[1, 0:1]), 1.0, 0.0)
    chunk[pl.ds(0, short.shape[0])] = short[...]
    chunk[pl.ds(short.shape[0], early)] = (pair[0] - rate_rows(sums, member) * pair[1]).astype(bf16)


def write_pass(sums, member, kept_master, kept_first, kept_second, kept_grad, kept_update,
               new_master, new_first, new_second, gathered, one, two, three, four, sems):
    rows = kept_master.shape[0]
    mine = pl.ds(pl.multiple_of(lax.axis_index("dp") * rows, rows), rows)
    copies = [
        pltpu.make_async_copy(source, target, sems.at[a]) for a, (source, target) in enumerate(
            ((one, new_first), (two, new_second), (three, new_master), (four, gathered.at[mine])))
    ]
    grad = kept_grad[...]
    one[...] = beta_first * kept_first[...] + (1.0 - beta_first) * grad
    copies[0].start()
    two[...] = beta_second * kept_second[...] + (1.0 - beta_second) * grad * grad
    copies[1].start()
    three[...] = kept_master[...] - rate_rows(sums, member[...]) * kept_update[...]
    copies[2].start()
    four[...] = three[...].astype(bf16)
    copies[3].start()
    for copy in copies:
        copy.wait()


def place_pass(chips, rows, items, before, *refs):
    pieces, (gathered, sems) = refs[:len(items)], refs[len(items):]
    core = lax.axis_index("dp") % 2
    copies = []
    for a, (step, swapped, first) in enumerate(items):
        owner = 2 * ring_owner(chips, step) + (1 - core if swapped else core)
        part = pl.ds(pl.multiple_of(owner * rows + first, 16), pieces[a].shape[0])
        copies.append(pltpu.make_async_copy(pieces[a], gathered.at[part], sems.at[a]))
        copies[-1].start()
    for copy in copies:
        copy.wait()


def place(chips, rows, items, gathered, *pieces):
    return pl.pallas_call(
        functools.partial(place_pass, chips, rows, items),
        out_shape=pltpu.HBM(gathered.shape, gathered.dtype),
        in_specs=[hbm] + [vmem] * len(items),
        out_specs=hbm,
        scratch_shapes=[pltpu.SemaphoreType.DMA((len(items),))],
        input_output_aliases={0: 0},
        compiler_params=pltpu.CompilerParams(vmem_limit_bytes=4 * MIB),
        name="place_pass",
    )(*in_hbm(gathered), *pieces)


def local(devices, dp, master, moment_first, moment_second, gradients, step_count, tensor_rows, decay_mask):
    rows, cols = master.shape
    kept = pltpu.VMEM((rows, cols), f32)
    early = rows // EARLY
    chips = dp // 2
    order = [2 * p if 2 * p < chips else 2 * (chips - p) - 1 for p in range(chips)]
    ring = [(2 * order[p] + c, 2 * order[(p + 1) % chips] + c) for p in range(chips) for c in range(2)]
    partner = [(d, d ^ 1) for d in range(dp)]
    small = [pltpu.SMEM(a.shape, a.dtype) for a in (tensor_rows, decay_mask)]

    kept_master, kept_first, kept_second, kept_grad, kept_update, member, bounds, pair, sums = pl.pallas_call(
        first_pass,
        out_shape=(kept,) * 5 + (
            pltpu.VMEM((rows, LANES), f32), pltpu.VMEM((2, TILE, LANES), jnp.int32), pltpu.VMEM((2, early, cols), f32),
            jax.ShapeDtypeStruct((devices, 2, LANES), f32)),
        in_specs=[pl.BlockSpec(memory_space=pltpu.SMEM)] + [hbm] * 6,
        out_specs=(vmem,) * 9,
        scratch_shapes=[pltpu.VMEM((rows, LANES), f32)] * 3 + small
        + [pltpu.SemaphoreType.DMA((2,)), pltpu.SemaphoreType.DMA((4, len(piece_sizes(rows))))],
        compiler_params=pltpu.CompilerParams(vmem_limit_bytes=4 * MIB),
        name="first_pass",
    )(step_count, *in_hbm(tensor_rows, decay_mask, master, moment_first, moment_second, gradients))

    pair = lax.ppermute(pair, "dp", ring)
    sums = lax.all_to_all(sums, ("dp", "mp"), 0, 0, tiled=True)

    sizes = [rows * share // sum(SHARES) for share in SHARES]
    firsts = [sum(sizes[:i]) for i in range(CHUNKS)]
    pieces = []
    for i in range(CHUNKS):
        shapes = (sizes[i],) if i < CHUNKS - 1 else (sizes[i], sizes[i] - early)
        pieces.append(pl.pallas_call(
            functools.partial(round_pass, firsts[i]),
            out_shape=tuple(pltpu.VMEM((size, cols), bf16) for size in shapes),
            in_specs=[vmem] * 4,
            out_specs=(vmem,) * len(shapes),
            compiler_params=pltpu.CompilerParams(vmem_limit_bytes=4 * MIB),
            name="round_pass",
        )(sums, member, kept_master, kept_update))

    new_master, new_first, new_second, gathered = pl.pallas_call(
        write_pass,
        out_shape=(jax.ShapeDtypeStruct((rows, cols), f32),) * 3 + (pltpu.HBM((dp * rows, cols), bf16),),
        in_specs=[vmem] * 7,
        out_specs=(hbm,) * 4,
        scratch_shapes=[pltpu.VMEM((rows, cols), f32)] * 3 + [pltpu.VMEM((rows, cols), bf16), pltpu.SemaphoreType.DMA((4,))],
        compiler_params=pltpu.CompilerParams(vmem_limit_bytes=24 * MIB),
        name="write_pass",
    )(sums, member, kept_master, kept_first, kept_second, kept_grad, kept_update)

    short = pieces[-1][1]
    pieces = [piece[0] for piece in pieces]
    others = []
    for k in range(chips):
        for i in range(CHUNKS):
            piece, first = pieces[i], firsts[i]
            if k < chips - 1:
                pieces[i] = lax.ppermute(short if (k, i) == (0, CHUNKS - 1) else piece, "dp", ring)
                if (k, i) == (0, CHUNKS - 1):
                    pieces[i] = pl.pallas_call(
                        functools.partial(merge_pass, chips, rows),
                        out_shape=pltpu.VMEM((sizes[i], cols), bf16),
                        in_specs=[vmem] * 4,
                        out_specs=vmem,
                        compiler_params=pltpu.CompilerParams(vmem_limit_bytes=4 * MIB),
                        name="merge_pass",
                    )(sums, bounds, pieces[i], pair)
            other = lax.ppermute(piece, "dp", partner)
            if k == 0:
                others.append(other)
                if i == CHUNKS - 1:
                    gathered = place(chips, rows, tuple((0, True, first) for first in firsts), gathered, *others)
            elif k == chips - 1 and i == CHUNKS - 1:
                gathered = place(chips, rows, ((k, False, first),), gathered, piece)
                gathered = place(chips, rows, ((k, True, first),), gathered, other)
            else:
                gathered = place(chips, rows, ((k, False, first), (k, True, first)), gathered, piece, other)
    return new_master, new_first, new_second, gathered


def solution(mesh):
    placed = (P("dp", "mp"), P("dp", "mp"), P("dp", "mp"), P("dp", "mp"), P(), P(), P())
    body = functools.partial(local, mesh.size, mesh.shape["dp"])

    return jax.shard_map(
        body,
        mesh=mesh,
        in_specs=placed,
        out_specs=(P("dp", "mp"), P("dp", "mp"), P("dp", "mp"), P(None, "mp")),
        check_vma=False,
    )
```
